256 devices in a mesh: robot: 64 (over x, z, core), sub: 4 (over y).
Axes of the slice: x: 4, y: 4, z: 8, core: 2. Of those that a mesh axis runs over, the one named last changes fastest.
Arguments:
- landmark_copies: float32 [64, 4, 3, 4096], P('robot', 'sub'), may hold values from -6 to 6
- dual_copies: float32 [64, 4, 3, 4096], P('robot', 'sub'), may hold values from -4 to 4
- visibility: int32 [64, 4, 4096], P('robot', 'sub'), may hold values from 0 to 511
- block_counts: int32 [64, 4, 64], P('robot', 'sub'), may hold values from 1 to 64, as said below
- consensus_old: float32 [64, 4, 3, 512], P('robot', 'sub'), may hold values from -6 to 6
- poses: float32 [64, 4, 6, 1024], P('robot', 'sub'), may hold values from -6 to 6
- inverse_blocks: float32 [64, 4, 36, 1024], P('robot', 'sub'), may hold values from -1.8 to 1.8
- jacobians: float32 [64, 4, 18, 4096], P('robot', 'sub'), may hold values from -3 to 3
- measurements: float32 [64, 4, 3, 4096], P('robot', 'sub'), may hold values from -6 to 6
- obs_pose: int32 [64, 4, 4096], P('robot', 'sub'), may hold values from 0 to 1023
- obs_slot: int32 [64, 4, 4096], P('robot', 'sub'), may hold values from 0 to 4095, as said below
- edge_to: int32 [64, 4, 1024], P('robot', 'sub'), may hold values from 0 to 4095
- edge_offset: float32 [64, 4, 6, 1024], P('robot', 'sub'), may hold values from -3 to 3
Outputs:
- refined_poses: float32 [64, 4, 6, 1024], P('robot', 'sub')
- consensus: float32 [64, 4, 3, 512], P('robot', 'sub')
- dual_new: float32 [64, 4, 3, 4096], P('robot', 'sub')
- residual_norms: float32 [2], replicated
The draws below stay inside these ranges and needn't reach their ends.
Inputs may be any that keep to these rules, and one draw needn't show every extreme that they name: block_counts[r,s,d] counts the live slots at the head of block d; for every sub index some robot receives full blocks from every robot, which robot varies with the draw. `obs_slot`: each observation names a live slot of its own device.
All inputs are finite; a program needn't handle non-finite values.
Results may differ from the reference program's by a relative error of at most 0.0001.
Values sent between devices are 32-bit elements; how exact they have to be, the bound alone decides.
A program may use at most 64 MiB of HBM per device.

```python
import math
import jax
import jax.numpy as jnp
import numpy as np
from jax import lax

LM_DEV = 512
CAP = 64
POSE_DEV = 1024
OBS_DEV = 4096
SLOTS = 4096
POSES = 4096
N_ROBOT = 64
N_SUB = 4


def count_table(key):
    base = jax.random.randint(jax.random.fold_in(key, 11), (N_ROBOT, N_SUB, N_ROBOT), 1, CAP // 2 + 1)
    heavy = jax.random.randint(jax.random.fold_in(key, 12), (1, N_SUB, 1), 0, N_ROBOT)
    target = jnp.arange(N_ROBOT, dtype=jnp.int32)[None, None, :]
    return jnp.where(target == heavy, CAP, base).astype(jnp.int32)


def draw_block_counts(key, part):
    return count_table(key)


def draw_obs_slot(key, part):
    counts = count_table(key)
    blocks = jax.random.randint(jax.random.fold_in(key, 13), (N_ROBOT, N_SUB, OBS_DEV), 0, N_ROBOT)
    picks = jax.random.randint(jax.random.fold_in(key, 14), (N_ROBOT, N_SUB, OBS_DEV), 0, CAP)
    limit = jnp.take_along_axis(counts, blocks, axis=2)
    return (blocks * CAP + picks % limit).astype(jnp.int32)


def with_ends(result, rng, least, high):
    dims = result.shape
    place = [jax.random.randint(jax.random.fold_in(rng, axis), (), 0, dims[axis]) for axis in range(len(dims))]
    result = result.at[tuple(place)].set(least)
    longest = dims.index(max(dims))
    place[longest] = (place[longest] + 1) % dims[longest]
    return result.at[tuple(place)].set(high)


def block_scale(rng, extent, cuts, least, largest):
    loudness, own = 1.0, jax.random.fold_in(rng, 6)
    for axis_at, shards_of in cuts:
        heights = jnp.exp(jax.random.uniform(jax.random.fold_in(own, axis_at), (shards_of,), jnp.float32, least / len(cuts), largest / len(cuts)))
        loudness = loudness * jnp.repeat(heights, extent[axis_at] // shards_of).reshape([-1 if axis == axis_at else 1 for axis in range(len(extent))])
    return loudness


def rank_table(amount, lean):
    portions = [(1 << 20) // math.isqrt(standing ** lean) + 1 for standing in range(1, amount + 1)]
    scale = 1 + sum(portions) // (1 << 30)
    return np.cumsum(np.array([max(1, weight // scale) for weight in portions]))


def skewed_ids(rng, dims, number_of, lean):
    table = rank_table(number_of, lean)
    ticket = jax.random.randint(jax.random.fold_in(rng, 1), dims, 0, int(table[number_of - 1]))
    standing = jnp.searchsorted(jnp.asarray(table, jnp.int32), ticket, side="right")
    return jax.random.permutation(jax.random.fold_in(rng, 2), number_of)[standing].astype(jnp.int32)


def scatter_about(stream_key, extent, width, bound, split=(), kind=jnp.bfloat16):
    values = width * jax.random.normal(stream_key, extent, jnp.float32)
    if split:
        values = values * block_scale(stream_key, extent, split, -0.22, 0.18)
    return jnp.clip(values, -bound, bound).astype(kind)


def setup_inputs(seed: int = 0) -> dict:
    key_list = jax.random.split(jax.random.key(seed), 14)
    landmark_copies = scatter_about(key_list[0], (N_ROBOT, N_SUB, 3, SLOTS), 1.0, 6.0, ((0, 64), (1, 4)), jnp.float32)
    dual_copies = scatter_about(key_list[1], (N_ROBOT, N_SUB, 3, SLOTS), 0.5, 4.0, ((0, 64), (1, 4)), jnp.float32)
    visibility = with_ends(skewed_ids(key_list[2], (N_ROBOT, N_SUB, SLOTS), LM_DEV, 2), jax.random.fold_in(key_list[2], 3), 0, LM_DEV - 1).astype(jnp.int32)
    block_counts = draw_block_counts(jax.random.fold_in(key_list[13], 71), 0)
    consensus_old = scatter_about(key_list[4], (N_ROBOT, N_SUB, 3, LM_DEV), 1.0, 6.0, ((0, 64), (1, 4)), jnp.float32)
    poses = scatter_about(key_list[5], (N_ROBOT, N_SUB, 6, POSE_DEV), 1.0, 6.0, ((0, 64), (1, 4)), jnp.float32)
    inverse_blocks = scatter_about(key_list[6], (N_ROBOT, N_SUB, 36, POSE_DEV), 0.3, 1.8, ((0, 64), (1, 4)), jnp.float32)
    jacobians = scatter_about(key_list[7], (N_ROBOT, N_SUB, 18, OBS_DEV), 0.5, 3.0, ((0, 64), (1, 4)), jnp.float32)
    measurements = scatter_about(key_list[8], (N_ROBOT, N_SUB, 3, OBS_DEV), 1.0, 6.0, ((0, 64), (1, 4)), jnp.float32)
    obs_pose = with_ends(jax.random.randint(key_list[9], (N_ROBOT, N_SUB, OBS_DEV), 0, POSE_DEV), jax.random.fold_in(key_list[9], 1), 0, POSE_DEV - 1).astype(jnp.int32)
    obs_slot = draw_obs_slot(jax.random.fold_in(key_list[13], 71), 0)
    edge_to = with_ends(jax.random.randint(key_list[11], (N_ROBOT, N_SUB, POSE_DEV), 0, POSES), jax.random.fold_in(key_list[11], 1), 0, POSES - 1).astype(jnp.int32)
    edge_offset = scatter_about(key_list[12], (N_ROBOT, N_SUB, 6, POSE_DEV), 0.5, 3.0, ((0, 64), (1, 4)), jnp.float32)
    return {"landmark_copies": landmark_copies, "dual_copies": dual_copies, "visibility": visibility, "block_counts": block_counts, "consensus_old": consensus_old, "poses": poses, "inverse_blocks": inverse_blocks, "jacobians": jacobians, "measurements": measurements, "obs_pose": obs_pose, "obs_slot": obs_slot, "edge_to": edge_to, "edge_offset": edge_offset}


penalty = 2.0

def reference(landmark_copies, dual_copies, visibility, block_counts, consensus_old, poses, inverse_blocks, jacobians, measurements, obs_pose, obs_slot, edge_to, edge_offset):
    robots = N_ROBOT
    subs = N_SUB
    live_mask = (jnp.arange(CAP)[None, None, None, :] < block_counts[..., None]).reshape(robots, subs, SLOTS).astype(jnp.float32)
    outgoing = (landmark_copies + dual_copies) * live_mask[:, :, None, :]
    target = (jnp.arange(SLOTS, dtype=jnp.int32) // CAP)[None, None, :] * LM_DEV + visibility
    sum_list = []
    seen_list = []
    for sub_index in range(subs):
        values = jnp.moveaxis(outgoing[:, sub_index], 1, 0).reshape(3, robots * SLOTS)
        flat_ids = target[:, sub_index].reshape(robots * SLOTS).astype(jnp.int32)
        summed = jax.vmap(lambda entries: jax.ops.segment_sum(entries, flat_ids, num_segments=robots * LM_DEV))(values)
        sum_list.append(jnp.moveaxis(summed.reshape(3, robots, LM_DEV), 0, 1))
        counted = jax.ops.segment_sum(live_mask[:, sub_index].reshape(robots * SLOTS), flat_ids, num_segments=robots * LM_DEV)
        seen_list.append(counted.reshape(robots, LM_DEV))
    totals = jnp.stack(sum_list, axis=1)
    seen = jnp.stack(seen_list, axis=1)
    consensus = (consensus_old + totals) / (1.0 + seen[:, :, None, :])
    back_list = []
    for sub_index in range(subs):
        flat = jnp.moveaxis(consensus[:, sub_index], 1, 0).reshape(3, robots * LM_DEV)
        picked = flat[:, target[:, sub_index]]
        back_list.append(jnp.moveaxis(picked, 1, 0))
    back = jnp.stack(back_list, axis=1)
    differ = (landmark_copies - back) * live_mask[:, :, None, :]
    dual_new = dual_copies + differ
    primal = jnp.sum(differ * differ)
    change = consensus - consensus_old
    dualsum = penalty * penalty * jnp.sum(seen[:, :, None, :] * change * change)
    residual_norms = jnp.sqrt(jnp.stack([primal, dualsum]) / (LM_DEV * robots * subs))
    copies_at = jnp.take_along_axis(landmark_copies, obs_slot[:, :, None, :], axis=3)
    error = measurements - copies_at
    jac_rows = jacobians.reshape(robots, subs, 3, 6, OBS_DEV)
    pull = lax.optimization_barrier(jnp.sum(jac_rows * error[:, :, :, None, :], axis=2))

    def pose_sums(rows, pose_ids):
        return jax.vmap(lambda entries: jax.ops.segment_sum(entries, pose_ids, num_segments=POSE_DEV))(rows)
    grad_obs = jax.vmap(jax.vmap(pose_sums))(pull, obs_pose)
    robot_all = jnp.moveaxis(poses, 1, 2).reshape(robots, 6, subs * POSE_DEV)
    pose_far = jax.vmap(lambda table, where: table[:, where])(robot_all, edge_to.reshape(robots, subs * POSE_DEV))
    pose_far = jnp.moveaxis(pose_far.reshape(robots, 6, subs, POSE_DEV), 2, 1)
    grad = grad_obs + pose_far - poses - edge_offset
    inverse = inverse_blocks.reshape(robots, subs, 6, 6, POSE_DEV)
    delta = lax.optimization_barrier(jnp.sum(inverse * grad[:, :, None, :, :], axis=3))
    return (poses + delta, consensus, dual_new, residual_norms)
```

```python
import functools

import jax
import jax.numpy as jnp
from jax import lax
from jax.experimental import pallas as pl
from jax.experimental.pallas import tpu as pltpu
from jax.sharding import PartitionSpec as P

MESH = pl.DeviceIdType.MESH
NX, NZ, SUBS = 4, 8, 4
CHIPS = NX * NZ
LANES = 128
PENALTY = 2.0
LANDMARKS = 131072.0
F32, BF16, I32 = jnp.float32, jnp.bfloat16, jnp.int32

OFFSETS = sorted(
    ((dx, dz) for dx in range(NX) for dz in range(NZ)),
    key=lambda o: (min(o[0], NX - o[0]) + min(o[1], NZ - o[1]), o),
)


def lane_gather(row, index):
    return jnp.take_along_axis(
        jnp.broadcast_to(row, index.shape), index, axis=1, mode="promise_in_bounds"
    )


def three_parts(x):
    high = x.astype(BF16).astype(F32)
    rest = x - high
    middle = rest.astype(BF16).astype(F32)
    return [high, middle, rest - middle]


def one_hot(lo_row):
    rows = lax.broadcasted_iota(I32, (LANES, LANES), 0)
    return jnp.where(rows == lo_row, 1.0, 0.0).astype(BF16)


def dot_entries(a, b):
    return lax.dot_general(a, b, (((1,), (1,)), ((), ())), preferred_element_type=F32)


def kernel(
    lc_h, dc_h, vis_h, cnt_h, cold_h, pose_h, inv_h, jac_h, meas_h, opose_h, oslot_h, edge_h, eoff_h,
    refined_h, cons_h, dual_h, norms_ref,
    lc, dc, vis, cnt, cold, pose, inv, jac, meas, opose, oslot, edge, eoff,
    send, recv, pull, totals, other_totals, other_cold, all_poses, returning, back, part, part1, part2,
    refined, cons, dual,
    load_sem, send_sem, recv_sem, y_send, y_recv, d2d_send, d2d_recv, ret_send, ret_recv,
    p1_send, p1_recv, p2_send, p2_recv, out_sem,
):
    robot, sub = lax.axis_index("robot"), lax.axis_index("sub")
    core, chip = lax.rem(robot, 2), lax.div(robot, 2)
    x, z = lax.div(chip, NZ), lax.rem(chip, NZ)

    loads = [
        pltpu.make_async_copy(src, dst, load_sem.at[i])
        for i, (src, dst) in enumerate(
            [(lc_h, lc), (dc_h, dc), (vis_h, vis), (cnt_h, cnt), (pose_h, pose), (cold_h, cold), (oslot_h, oslot),
             (meas_h, meas), (jac_h, jac), (opose_h, opose), (edge_h, edge), (eoff_h, eoff), (inv_h, inv)]
        )
    ]
    for load in loads:
        load.start()

    def at_offset(k, sign=1):
        dx, dz = OFFSETS[k]
        px = lax.rem(x + (dx if sign > 0 else NX - dx), NX)
        pz = lax.rem(z + (dz if sign > 0 else NZ - dz), NZ)
        return px * NZ + pz

    group = [(dc_, ds) for dc_ in range(2) for ds in range(SUBS) if (dc_, ds) != (0, 0)]

    def group_peer(dc_, ds):
        return {
            "robot": chip * 2 + lax.rem(core + dc_, 2),
            "sub": lax.rem(sub + ds, SUBS),
        }

    barrier = pltpu.get_barrier_semaphore()
    for k in range(1, CHIPS):
        pl.semaphore_signal(
            barrier,
            inc=1,
            device_id={"robot": at_offset(k) * 2 + core, "sub": sub},
            device_id_type=MESH,
        )
    for dc_, ds in group:
        pl.semaphore_signal(
            barrier, inc=1, device_id=group_peer(dc_, ds), device_id_type=MESH
        )

    for i in range(4):
        loads[i].wait()
    lane = lax.broadcasted_iota(I32, (CHIPS, LANES), 1)
    counts = jnp.broadcast_to(cnt[...].astype(F32), (CHIPS, 64))
    at = lax.broadcasted_iota(I32, (CHIPS, 64), 1)
    row2 = lax.broadcasted_iota(I32, (CHIPS, 64), 0) * 2
    even = jnp.sum(jnp.where(at == row2, counts, 0.0), axis=1, keepdims=True)
    odd = jnp.sum(jnp.where(at == row2 + 1, counts, 0.0), axis=1, keepdims=True)
    limit = jnp.where(lane < 64, even, odd)
    live = jnp.where((lane & 63).astype(F32) < limit, 1.0, 0.0)
    for v in range(3):
        send[:, v, :] = lc[v]
        send[:, 3 + v, :] = (lc[v] + dc[v]) * live
    send[:, 6, :] = live
    send[:, 7, :] = vis[...].astype(F32)
    recv[0] = send[chip]
    loads[4].wait()
    all_poses[sub] = pose[...]
    loads[5].wait()

    pl.semaphore_wait(barrier, CHIPS - 1 + len(group))

    def exchange(k):
        peer = at_offset(k)
        return pltpu.make_async_remote_copy(
            src_ref=send.at[peer],
            dst_ref=recv.at[k],
            send_sem=send_sem,
            recv_sem=recv_sem.at[k],
            device_id={"robot": peer * 2 + core, "sub": sub},
            device_id_type=MESH,
        )

    for k in range(CHIPS - 1, 0, -1):
        exchange(k).start()
    y_copies = [
        pltpu.make_async_remote_copy(
            src_ref=pose,
            dst_ref=all_poses.at[sub],
            send_sem=y_send.at[ds - 1],
            recv_sem=y_recv.at[ds - 1],
            device_id={"robot": robot, "sub": lax.rem(sub + ds, SUBS)},
            device_id_type=MESH,
        )
        for ds in range(1, SUBS)
    ]
    for copy in y_copies:
        copy.start()
    partner = group_peer(1, 0)
    cold_copy = pltpu.make_async_remote_copy(
        src_ref=cold,
        dst_ref=other_cold,
        send_sem=d2d_send.at[0],
        recv_sem=d2d_recv.at[0],
        device_id=partner,
        device_id_type=MESH,
    )
    cold_copy.start()

    loads[6].wait()
    blocks = [slice(8 * b, 8 * b + 8) for b in range(4)]
    slot_lo = [oslot[b, :] & 127 for b in blocks]
    slot_hi = [oslot[b, :] >> 7 for b in blocks]

    def gather_copies(h, found):
        new = []
        for v in range(3):
            row = lc[v, pl.ds(h, 1), :]
            for b in range(4):
                new.append(jnp.where(slot_hi[b] == h, lane_gather(row, slot_lo[b]), found[4 * v + b]))
        return tuple(new)

    zero = jnp.zeros((8, LANES), F32)
    found = lax.fori_loop(0, 32, gather_copies, (zero,) * 12, unroll=4)
    for i in (7, 8, 9):
        loads[i].wait()
    for b in range(4):
        error = [meas[v, blocks[b], :] - found[4 * v + b] for v in range(3)]
        for a in range(6):
            pull[a, blocks[b], :] = sum(jac[6 * k + a, blocks[b], :] * error[k] for k in range(3))

    sub8 = lax.broadcasted_iota(I32, (8, LANES), 0)

    def pose_step(i, acc):
        left, right = [], []
        for j in range(2):
            t = 2 * i + j
            ids = opose[pl.ds(t, 1), :]
            mask = jnp.broadcast_to(ids >> 7, (8, LANES)) == sub8
            rows = []
            for a in range(6):
                value = jnp.broadcast_to(pull[a, pl.ds(t, 1), :], (8, LANES))
                rows += three_parts(jnp.where(mask, value, 0.0))
            left.append(jnp.concatenate(rows, axis=0).astype(BF16))
            right.append(one_hot(ids & 127))
        return acc + dot_entries(jnp.concatenate(left, axis=1), jnp.concatenate(right, axis=1))

    pose_acc = lax.fori_loop(0, 16, pose_step, jnp.zeros((144, LANES), F32), unroll=2)
    for i in (10, 11, 12):
        loads[i].wait()
    for a in range(6):
        base = 24 * a
        grad_obs = pose_acc[base : base + 8] + pose_acc[base + 8 : base + 16] + pose_acc[base + 16 : base + 24]
        refined[a] = grad_obs - pose[a] - eoff[a]

    half = lax.broadcasted_iota(I32, (8, LANES), 1) >> 6
    shift = jnp.where(half == core, 0, 4)

    def landmark_pair(ks):
        left, right = [], []
        for k in ks:
            ids = recv[k, 7:8, :].astype(I32)
            mask = jnp.broadcast_to(ids >> 7, (8, LANES)) + shift == sub8
            rows = []
            for v in range(3):
                value = jnp.broadcast_to(recv[k, 3 + v : 4 + v, :], (8, LANES))
                rows += three_parts(jnp.where(mask, value, 0.0))
            rows.append(jnp.where(mask, jnp.broadcast_to(recv[k, 6:7, :], (8, LANES)), 0.0))
            left.append(jnp.concatenate(rows, axis=0).astype(BF16))
            right.append(one_hot(ids & 127))
        return dot_entries(jnp.concatenate(left, axis=1), jnp.concatenate(right, axis=1))

    acc = jnp.zeros((80, LANES), F32)
    for i in range(CHIPS // 2):
        for k in (2 * i, 2 * i + 1):
            if k:
                exchange(k).wait_recv()
        acc = acc + landmark_pair((2 * i, 2 * i + 1))
    for v in range(3):
        base = 24 * v
        totals[v] = acc[base : base + 8] + acc[base + 8 : base + 16] + acc[base + 16 : base + 24]
    totals[3] = acc[72:80]
    totals_copy = pltpu.make_async_remote_copy(
        src_ref=totals,
        dst_ref=other_totals,
        send_sem=d2d_send.at[1],
        recv_sem=d2d_recv.at[1],
        device_id=partner,
        device_id_type=MESH,
    )
    totals_copy.start()
    cold_copy.wait_recv()
    totals_copy.wait_recv()

    def swapped(q):
        return jnp.concatenate([other_totals[q, 4:8, :], other_totals[q, 0:4, :]], axis=0)

    seen = totals[3] + swapped(3)
    estimate = []
    dual_part = jnp.zeros((8, LANES), F32)
    for v in range(3):
        old = jnp.concatenate([cold[v], other_cold[v]], axis=0)
        new = (old + totals[v] + swapped(v)) / (1.0 + seen)
        estimate.append(new)
        cons[v] = new[0:4]
        change = new - old
        dual_part = dual_part + jnp.where(sub8 < 4, seen * change * change, 0.0)
    cons_out = pltpu.make_async_copy(cons, cons_h, out_sem.at[0])
    cons_out.start()

    def give_back(k):
        peer = at_offset(k, -1)
        return pltpu.make_async_remote_copy(
            src_ref=returning.at[k],
            dst_ref=back.at[chip],
            send_sem=ret_send,
            recv_sem=ret_recv,
            device_id={"robot": peer * 2 + core, "sub": sub},
            device_id_type=MESH,
        )

    primal_part = jnp.zeros((8, LANES), F32)
    for b in (3, 2, 1, 0):
        ks = blocks[b]
        ids = recv[ks, 7, :].astype(I32)
        lo, hi = ids & 127, (ids >> 7) + shift
        alive = recv[ks, 6, :]
        for v in range(3):
            value = jnp.zeros((8, LANES), F32)
            for h in range(8):
                value = jnp.where(hi == h, lane_gather(estimate[v][h : h + 1], lo), value)
            returning[ks, v, :] = value
            differ = alive * (recv[ks, v, :] - value)
            primal_part = primal_part + differ * differ
        returning[ks, 3, :] = alive
        for k in range(8 * b + 7, 8 * b - 1, -1):
            if k:
                give_back(k).start()

    part[0:1, :] = jnp.sum(primal_part, axis=0, keepdims=True)
    part[1:2, :] = PENALTY * PENALTY * jnp.sum(dual_part, axis=0, keepdims=True)
    mine = sub * 2 + core
    p1 = [
        pltpu.make_async_remote_copy(
            src_ref=part,
            dst_ref=part1.at[mine],
            send_sem=p1_send,
            recv_sem=p1_recv,
            device_id=group_peer(dc_, ds),
            device_id_type=MESH,
        )
        for dc_, ds in group
    ]
    for copy in p1:
        copy.start()
    part1[mine] = part[...]
    back[chip] = returning[0]

    for copy in y_copies:
        copy.wait_recv()
    edge_lo, edge_hi = edge[...] & 127, edge[...] >> 7

    def gather_poses(h, far):
        new = []
        for a in range(6):
            row = all_poses[lax.div(h, 8), a, pl.ds(lax.rem(h, 8), 1), :]
            new.append(jnp.where(edge_hi == h, lane_gather(row, edge_lo), far[a]))
        return tuple(new)

    far = lax.fori_loop(0, 32, gather_poses, (zero,) * 6, unroll=4)
    grad = [refined[a] + far[a] for a in range(6)]
    for a in range(6):
        refined[a] = pose[a] + sum(inv[6 * a + b] * grad[b] for b in range(6))
    refined_out = pltpu.make_async_copy(refined, refined_h, out_sem.at[1])
    refined_out.start()

    pltpu.make_async_copy(part1.at[pl.ds(0, 7)], part1.at[pl.ds(0, 7)], p1_recv).wait()
    summed = part1[0]
    for i in range(1, 8):
        summed = summed + part1[i]
    part2[chip] = summed
    p2 = [
        pltpu.make_async_remote_copy(
            src_ref=part2.at[chip],
            dst_ref=part2.at[chip],
            send_sem=p2_send,
            recv_sem=p2_recv,
            device_id={"robot": at_offset(k) * 2 + core, "sub": sub},
            device_id_type=MESH,
        )
        for k in range(CHIPS - 1, 0, -1)
    ]
    for copy in p2:
        copy.start()

    pltpu.make_async_copy(back.at[pl.ds(0, CHIPS - 1)], back.at[pl.ds(0, CHIPS - 1)], ret_recv).wait()
    for b in blocks:
        alive = send[b, 6, :]
        for v in range(3):
            dual[v, b, :] = dc[v, b, :] + alive * (lc[v, b, :] - back[b, v, :])
    dual_out = pltpu.make_async_copy(dual, dual_h, out_sem.at[2])
    dual_out.start()

    pltpu.make_async_copy(part2.at[pl.ds(0, CHIPS - 1)], part2.at[pl.ds(0, CHIPS - 1)], p2_recv).wait()
    total = part2[0]
    for i in range(1, CHIPS):
        total = total + part2[i]
    total = jnp.sum(total, axis=1, keepdims=True)
    norms = jnp.sqrt(total / LANDMARKS)
    norms_ref[...] = jnp.broadcast_to(norms, (2, LANES))

    pltpu.make_async_copy(send.at[pl.ds(0, CHIPS - 1)], send.at[pl.ds(0, CHIPS - 1)], send_sem).wait()
    pltpu.make_async_copy(returning.at[pl.ds(0, CHIPS - 1)], returning.at[pl.ds(0, CHIPS - 1)], ret_send).wait()
    pltpu.make_async_copy(part1.at[pl.ds(0, 7)], part1.at[pl.ds(0, 7)], p1_send).wait()
    pltpu.make_async_copy(part2.at[pl.ds(0, CHIPS - 1)], part2.at[pl.ds(0, CHIPS - 1)], p2_send).wait()
    for copy in y_copies:
        copy.wait_send()
    cold_copy.wait_send()
    totals_copy.wait_send()
    cons_out.wait()
    refined_out.wait()
    dual_out.wait()


SHAPES = [
    ((3, 32, 128), F32), ((3, 32, 128), F32), ((32, 128), I32), ((1, 64), I32), ((3, 4, 128), F32), ((6, 8, 128), F32),
    ((36, 8, 128), F32), ((18, 32, 128), F32), ((3, 32, 128), F32), ((32, 128), I32), ((32, 128), I32), ((8, 128), I32),
    ((6, 8, 128), F32),
]


def body(*args):
    given = [a.reshape(shape) for a, (shape, _) in zip(args, SHAPES, strict=True)]
    anywhere = pl.BlockSpec(memory_space=pl.ANY)
    dma, vmem = pltpu.SemaphoreType.DMA, pltpu.VMEM
    refined, cons, dual, norms = pl.pallas_call(
        kernel,
        out_shape=(
            jax.ShapeDtypeStruct((6, 8, 128), F32),
            jax.ShapeDtypeStruct((3, 4, 128), F32),
            jax.ShapeDtypeStruct((3, 32, 128), F32),
            jax.ShapeDtypeStruct((2, 128), F32),
        ),
        in_specs=[anywhere] * 13,
        out_specs=(anywhere, anywhere, anywhere, pl.BlockSpec(memory_space=vmem)),
        scratch_shapes=[
            *[vmem(shape, dtype) for shape, dtype in SHAPES],
            vmem((CHIPS, 8, LANES), F32),
            vmem((CHIPS, 8, LANES), F32),
            vmem((6, 32, LANES), F32),
            vmem((4, 8, LANES), F32),
            vmem((4, 8, LANES), F32),
            vmem((3, 4, LANES), F32),
            vmem((SUBS, 6, 8, LANES), F32),
            vmem((CHIPS, 4, LANES), F32),
            vmem((CHIPS, 4, LANES), F32),
            vmem((2, LANES), F32),
            vmem((8, 2, LANES), F32),
            vmem((CHIPS, 2, LANES), F32),
            vmem((6, 8, LANES), F32),
            vmem((3, 4, LANES), F32),
            vmem((3, 32, LANES), F32),
            dma((13,)), dma, dma((CHIPS,)), dma((3,)), dma((3,)), dma((2,)), dma((2,)), dma, dma, dma, dma, dma, dma,
            dma((3,)),
        ],
        compiler_params=pltpu.CompilerParams(collective_id=0, has_side_effects=True),
    )(*given)
    return (
        refined.reshape(1, 1, 6, 1024),
        cons.reshape(1, 1, 3, 512),
        dual.reshape(1, 1, 3, 4096),
        norms[:, 0],
    )


def solution(mesh):
    three, four = P("robot", "sub", None), P("robot", "sub", None, None)
    return jax.shard_map(
        body,
        mesh=mesh,
        in_specs=(four, four, three, three, four, four, four, four, four, three, three, three, four),
        out_specs=(four, four, four, P()),
        check_vma=False,
    )
```

```python
import functools

import jax
import jax.numpy as jnp
from jax import lax
from jax.experimental import pallas as pl
from jax.experimental.pallas import tpu as pltpu
from jax.sharding import PartitionSpec as P

MESH = pl.DeviceIdType.MESH
NX, NZ, SUBS = 4, 8, 4
CHIPS = NX * NZ
LANES = 128
PENALTY = 2.0
LANDMARKS = 131072.0
F32, BF16, I32 = jnp.float32, jnp.bfloat16, jnp.int32

OFFSETS = sorted(
    ((dx, dz) for dx in range(NX) for dz in range(NZ)),
    key=lambda o: (min(o[0], NX - o[0]) + min(o[1], NZ - o[1]), o),
)


def lane_gather(row, index):
    return jnp.take_along_axis(
        jnp.broadcast_to(row, index.shape), index, axis=1, mode="promise_in_bounds"
    )


def three_parts(x):
    high = x.astype(BF16).astype(F32)
    rest = x - high
    middle = rest.astype(BF16).astype(F32)
    return [high, middle, rest - middle]


def one_hot(lo_row):
    rows = lax.broadcasted_iota(I32, (LANES, LANES), 0)
    return jnp.where(rows == lo_row, 1.0, 0.0).astype(BF16)


def dot_entries(a, b):
    return lax.dot_general(a, b, (((1,), (1,)), ((), ())), preferred_element_type=F32)


def kernel(
    lc_h, dc_h, vis_h, cnt_h, cold_h, pose_h, inv_h, jac_h, meas_h, opose_h, oslot_h, edge_h, eoff_h,
    refined, cons, dual, norms_ref,
    lc, dc, vis, cnt, cold, pose, inv, jac, meas, opose, oslot, edge, eoff,
    send, recv, pull, totals, other_totals, other_cold, all_poses, returning, back, part, part1, part2,
    load_sem, send_sem, recv_sem, y_send, y_recv, d2d_send, d2d_recv, ret_send, ret_recv,
    p1_send, p1_recv, p2_send, p2_recv,
):
    robot, sub = lax.axis_index("robot"), lax.axis_index("sub")
    core, chip = lax.rem(robot, 2), lax.div(robot, 2)
    x, z = lax.div(chip, NZ), lax.rem(chip, NZ)

    def at_offset(k, sign=1):
        dx, dz = OFFSETS[k]
        px = lax.rem(x + (dx if sign > 0 else NX - dx), NX)
        pz = lax.rem(z + (dz if sign > 0 else NZ - dz), NZ)
        return px * NZ + pz

    group = [(dc_, ds) for dc_ in range(2) for ds in range(SUBS) if (dc_, ds) != (0, 0)]

    def group_peer(dc_, ds):
        return {
            "robot": chip * 2 + lax.rem(core + dc_, 2),
            "sub": lax.rem(sub + ds, SUBS),
        }

    barrier = pltpu.get_barrier_semaphore()
    for k in range(CHIPS - 1, 0, -1):
        pl.semaphore_signal(
            barrier,
            inc=1,
            device_id={"robot": at_offset(k) * 2 + core, "sub": sub},
            device_id_type=MESH,
        )
    for dc_, ds in group:
        pl.semaphore_signal(
            barrier, inc=1, device_id=group_peer(dc_, ds), device_id_type=MESH
        )

    loads = [
        pltpu.make_async_copy(src, dst, load_sem.at[i])
        for i, (src, dst) in enumerate(
            [(lc_h, lc), (dc_h, dc), (vis_h, vis), (cnt_h, cnt), (pose_h, pose), (cold_h, cold), (oslot_h, oslot),
             (meas_h, meas), (jac_h, jac), (opose_h, opose), (edge_h, edge), (eoff_h, eoff), (inv_h, inv)]
        )
    ]
    for load in loads:
        load.start()

    for i in range(4):
        loads[i].wait()
    lane = lax.broadcasted_iota(I32, (CHIPS, LANES), 1)
    counts = jnp.broadcast_to(cnt[...].astype(F32), (CHIPS, 64))
    at = lax.broadcasted_iota(I32, (CHIPS, 64), 1)
    row2 = lax.broadcasted_iota(I32, (CHIPS, 64), 0) * 2
    even = jnp.sum(jnp.where(at == row2, counts, 0.0), axis=1, keepdims=True)
    odd = jnp.sum(jnp.where(at == row2 + 1, counts, 0.0), axis=1, keepdims=True)
    limit = jnp.where(lane < 64, even, odd)
    live = jnp.where((lane & 63).astype(F32) < limit, 1.0, 0.0)
    for v in range(3):
        send[:, v, :] = lc[v]
        send[:, 3 + v, :] = (lc[v] + dc[v]) * live
    send[:, 6, :] = live
    send[:, 7, :] = vis[...].astype(F32)
    recv[0] = send[chip]
    loads[4].wait()
    all_poses[sub] = pose[...]
    loads[5].wait()

    loads[6].wait()
    blocks = [slice(8 * b, 8 * b + 8) for b in range(4)]
    slot_lo = [oslot[b, :] & 127 for b in blocks]
    slot_hi = [oslot[b, :] >> 7 for b in blocks]

    def gather_copies(h, found):
        new = []
        for v in range(3):
            row = lc[v, pl.ds(h, 1), :]
            for b in range(4):
                new.append(jnp.where(slot_hi[b] == h, lane_gather(row, slot_lo[b]), found[4 * v + b]))
        return tuple(new)

    zero = jnp.zeros((8, LANES), F32)
    found = lax.fori_loop(0, 32, gather_copies, (zero,) * 12, unroll=4)
    for i in (7, 8, 9):
        loads[i].wait()
    for b in range(4):
        error = [meas[v, blocks[b], :] - found[4 * v + b] for v in range(3)]
        for a in range(6):
            pull[a, blocks[b], :] = sum(jac[6 * k + a, blocks[b], :] * error[k] for k in range(3))

    pl.semaphore_wait(barrier, CHIPS - 1 + len(group))

    def exchange(k):
        peer = at_offset(k)
        return pltpu.make_async_remote_copy(
            src_ref=send.at[peer],
            dst_ref=recv.at[k],
            send_sem=send_sem,
            recv_sem=recv_sem.at[k],
            device_id={"robot": peer * 2 + core, "sub": sub},
            device_id_type=MESH,
        )

    for k in range(CHIPS - 1, 0, -1):
        exchange(k).start()
    y_copies = [
        pltpu.make_async_remote_copy(
            src_ref=pose,
            dst_ref=all_poses.at[sub],
            send_sem=y_send.at[ds - 1],
            recv_sem=y_recv.at[ds - 1],
            device_id={"robot": robot, "sub": lax.rem(sub + ds, SUBS)},
            device_id_type=MESH,
        )
        for ds in range(1, SUBS)
    ]
    for copy in y_copies:
        copy.start()
    partner = group_peer(1, 0)
    cold_copy = pltpu.make_async_remote_copy(
        src_ref=cold,
        dst_ref=other_cold,
        send_sem=d2d_send.at[0],
        recv_sem=d2d_recv.at[0],
        device_id=partner,
        device_id_type=MESH,
    )
    cold_copy.start()

    sub8 = lax.broadcasted_iota(I32, (8, LANES), 0)

    def pose_step(i, acc):
        left, right = [], []
        for j in range(2):
            t = 2 * i + j
            ids = opose[pl.ds(t, 1), :]
            mask = jnp.broadcast_to(ids >> 7, (8, LANES)) == sub8
            rows = []
            for a in range(6):
                value = jnp.broadcast_to(pull[a, pl.ds(t, 1), :], (8, LANES))
                rows += three_parts(jnp.where(mask, value, 0.0))
            left.append(jnp.concatenate(rows, axis=0).astype(BF16))
            right.append(one_hot(ids & 127))
        return acc + dot_entries(jnp.concatenate(left, axis=1), jnp.concatenate(right, axis=1))

    pose_acc = lax.fori_loop(0, 16, pose_step, jnp.zeros((144, LANES), F32), unroll=2)
    for i in (10, 11, 12):
        loads[i].wait()
    for a in range(6):
        base = 24 * a
        grad_obs = pose_acc[base : base + 8] + pose_acc[base + 8 : base + 16] + pose_acc[base + 16 : base + 24]
        refined[a] = grad_obs - pose[a] - eoff[a]

    half = lax.broadcasted_iota(I32, (8, LANES), 1) >> 6
    shift = jnp.where(half == core, 0, 4)

    def landmark_pair(ks):
        left, right = [], []
        for k in ks:
            ids = recv[k, 7:8, :].astype(I32)
            mask = jnp.broadcast_to(ids >> 7, (8, LANES)) + shift == sub8
            rows = []
            for v in range(3):
                value = jnp.broadcast_to(recv[k, 3 + v : 4 + v, :], (8, LANES))
                rows += three_parts(jnp.where(mask, value, 0.0))
            rows.append(jnp.where(mask, jnp.broadcast_to(recv[k, 6:7, :], (8, LANES)), 0.0))
            left.append(jnp.concatenate(rows, axis=0).astype(BF16))
            right.append(one_hot(ids & 127))
        return dot_entries(jnp.concatenate(left, axis=1), jnp.concatenate(right, axis=1))

    acc = jnp.zeros((80, LANES), F32)
    for i in range(CHIPS // 2):
        for k in (2 * i, 2 * i + 1):
            if k:
                exchange(k).wait_recv()
        acc = acc + landmark_pair((2 * i, 2 * i + 1))
    for v in range(3):
        base = 24 * v
        totals[v] = acc[base : base + 8] + acc[base + 8 : base + 16] + acc[base + 16 : base + 24]
    totals[3] = acc[72:80]
    totals_copy = pltpu.make_async_remote_copy(
        src_ref=totals,
        dst_ref=other_totals,
        send_sem=d2d_send.at[1],
        recv_sem=d2d_recv.at[1],
        device_id=partner,
        device_id_type=MESH,
    )
    totals_copy.start()
    cold_copy.wait_recv()
    totals_copy.wait_recv()

    def swapped(q):
        return jnp.concatenate([other_totals[q, 4:8, :], other_totals[q, 0:4, :]], axis=0)

    seen = totals[3] + swapped(3)
    estimate = []
    dual_part = jnp.zeros((8, LANES), F32)
    for v in range(3):
        old = jnp.concatenate([cold[v], other_cold[v]], axis=0)
        new = (old + totals[v] + swapped(v)) / (1.0 + seen)
        estimate.append(new)
        cons[v] = new[0:4]
        change = new - old
        dual_part = dual_part + jnp.where(sub8 < 4, seen * change * change, 0.0)
    def give_back(k):
        peer = at_offset(k, -1)
        return pltpu.make_async_remote_copy(
            src_ref=returning.at[k],
            dst_ref=back.at[chip],
            send_sem=ret_send,
            recv_sem=ret_recv,
            device_id={"robot": peer * 2 + core, "sub": sub},
            device_id_type=MESH,
        )

    primal_part = jnp.zeros((8, LANES), F32)
    for b in (3, 2, 1, 0):
        ks = blocks[b]
        ids = recv[ks, 7, :].astype(I32)
        lo, hi = ids & 127, (ids >> 7) + shift
        alive = recv[ks, 6, :]
        for v in range(3):
            value = jnp.zeros((8, LANES), F32)
            for h in range(8):
                value = jnp.where(hi == h, lane_gather(estimate[v][h : h + 1], lo), value)
            returning[ks, v, :] = value
            differ = alive * (recv[ks, v, :] - value)
            primal_part = primal_part + differ * differ
        returning[ks, 3, :] = alive
        for k in range(8 * b + 7, 8 * b - 1, -1):
            if k:
                give_back(k).start()

    part[0:1, :] = jnp.sum(primal_part, axis=0, keepdims=True)
    part[1:2, :] = PENALTY * PENALTY * jnp.sum(dual_part, axis=0, keepdims=True)
    mine = sub * 2 + core
    p1 = [
        pltpu.make_async_remote_copy(
            src_ref=part,
            dst_ref=part1.at[mine],
            send_sem=p1_send,
            recv_sem=p1_recv,
            device_id=group_peer(dc_, ds),
            device_id_type=MESH,
        )
        for dc_, ds in group
    ]
    for copy in p1:
        copy.start()
    part1[mine] = part[...]
    back[chip] = returning[0]

    for copy in y_copies:
        copy.wait_recv()
    edge_lo, edge_hi = edge[...] & 127, edge[...] >> 7

    def gather_poses(h, far):
        new = []
        for a in range(6):
            row = all_poses[lax.div(h, 8), a, pl.ds(lax.rem(h, 8), 1), :]
            new.append(jnp.where(edge_hi == h, lane_gather(row, edge_lo), far[a]))
        return tuple(new)

    far = lax.fori_loop(0, 32, gather_poses, (zero,) * 6, unroll=4)
    grad = [refined[a] + far[a] for a in range(6)]
    for a in range(6):
        refined[a] = pose[a] + sum(inv[6 * a + b] * grad[b] for b in range(6))

    pltpu.make_async_copy(part1.at[pl.ds(0, 7)], part1.at[pl.ds(0, 7)], p1_recv).wait()
    summed = part1[0]
    for i in range(1, 8):
        summed = summed + part1[i]
    part2[chip] = summed
    p2 = [
        pltpu.make_async_remote_copy(
            src_ref=part2.at[chip],
            dst_ref=part2.at[chip],
            send_sem=p2_send,
            recv_sem=p2_recv,
            device_id={"robot": at_offset(k) * 2 + core, "sub": sub},
            device_id_type=MESH,
        )
        for k in range(CHIPS - 1, 0, -1)
    ]
    for copy in p2:
        copy.start()

    pltpu.make_async_copy(back.at[pl.ds(0, CHIPS - 1)], back.at[pl.ds(0, CHIPS - 1)], ret_recv).wait()
    for b in blocks:
        alive = send[b, 6, :]
        for v in range(3):
            dual[v, b, :] = dc[v, b, :] + alive * (lc[v, b, :] - back[b, v, :])

    pltpu.make_async_copy(part2.at[pl.ds(0, CHIPS - 1)], part2.at[pl.ds(0, CHIPS - 1)], p2_recv).wait()
    total = part2[0]
    for i in range(1, CHIPS):
        total = total + part2[i]
    total = jnp.sum(total, axis=1, keepdims=True)
    norms = jnp.broadcast_to(jnp.sqrt(total / LANDMARKS), (2, LANES))
    norms_ref[...] = jnp.where(lax.broadcasted_iota(I32, (1, LANES), 1) == 0, norms[0:1], norms[1:2])

    pltpu.make_async_copy(send.at[pl.ds(0, CHIPS - 1)], send.at[pl.ds(0, CHIPS - 1)], send_sem).wait()
    pltpu.make_async_copy(returning.at[pl.ds(0, CHIPS - 1)], returning.at[pl.ds(0, CHIPS - 1)], ret_send).wait()
    pltpu.make_async_copy(part1.at[pl.ds(0, 7)], part1.at[pl.ds(0, 7)], p1_send).wait()
    pltpu.make_async_copy(part2.at[pl.ds(0, CHIPS - 1)], part2.at[pl.ds(0, CHIPS - 1)], p2_send).wait()
    for copy in y_copies:
        copy.wait_send()
    cold_copy.wait_send()
    totals_copy.wait_send()


SHAPES = [
    ((3, 32, 128), F32), ((3, 32, 128), F32), ((32, 128), I32), ((1, 64), I32), ((3, 4, 128), F32), ((6, 8, 128), F32),
    ((36, 8, 128), F32), ((18, 32, 128), F32), ((3, 32, 128), F32), ((32, 128), I32), ((32, 128), I32), ((8, 128), I32),
    ((6, 8, 128), F32),
]

OUT_SHAPES = [(6, 8, 128), (3, 4, 128), (3, 32, 128), (1, 128)]


def write_out(refined, cons, dual, norms, refined_h, cons_h, dual_h, norms_out, sem):
    copies = [
        pltpu.make_async_copy(src, dst, sem.at[i])
        for i, (src, dst) in enumerate([(dual, dual_h), (refined, refined_h), (cons, cons_h)])
    ]
    for copy in copies:
        copy.start()
    norms_out[...] = norms[:, 0:2]
    for copy in copies:
        copy.wait()


def body(*args):
    given = [a.reshape(shape) for a, (shape, _) in zip(args, SHAPES, strict=True)]
    anywhere = pl.BlockSpec(memory_space=pl.ANY)
    dma, vmem = pltpu.SemaphoreType.DMA, pltpu.VMEM
    results = pl.pallas_call(
        kernel,
        out_shape=tuple(vmem(shape, F32) for shape in OUT_SHAPES),
        in_specs=[anywhere] * 13,
        out_specs=(pl.BlockSpec(memory_space=vmem),) * 4,
        scratch_shapes=[
            *[vmem(shape, dtype) for shape, dtype in SHAPES],
            vmem((CHIPS, 8, LANES), F32),
            vmem((CHIPS, 8, LANES), F32),
            vmem((6, 32, LANES), F32),
            vmem((4, 8, LANES), F32),
            vmem((4, 8, LANES), F32),
            vmem((3, 4, LANES), F32),
            vmem((SUBS, 6, 8, LANES), F32),
            vmem((CHIPS, 4, LANES), F32),
            vmem((CHIPS, 4, LANES), F32),
            vmem((2, LANES), F32),
            vmem((8, 2, LANES), F32),
            vmem((CHIPS, 2, LANES), F32),
            dma((13,)), dma, dma((CHIPS,)), dma((3,)), dma((3,)), dma((2,)), dma((2,)), dma, dma, dma, dma, dma, dma,
        ],
        compiler_params=pltpu.CompilerParams(collective_id=0, has_side_effects=True),
    )(*given)
    refined, cons, dual, norms = pl.pallas_call(
        write_out,
        out_shape=tuple(jax.ShapeDtypeStruct(shape, F32) for shape in OUT_SHAPES[:3] + [(1, 2)]),
        in_specs=[pl.BlockSpec(memory_space=vmem)] * 4,
        out_specs=(anywhere, anywhere, anywhere, pl.BlockSpec(memory_space=vmem)),
        scratch_shapes=[dma((3,))],
    )(*[pltpu.with_memory_space_constraint(r, vmem) for r in results])
    return (
        refined.reshape(1, 1, 6, 1024),
        cons.reshape(1, 1, 3, 512),
        dual.reshape(1, 1, 3, 4096),
        norms.reshape(2),
    )


def solution(mesh):
    three, four = P("robot", "sub", None), P("robot", "sub", None, None)
    return jax.shard_map(
        body,
        mesh=mesh,
        in_specs=(four, four, three, three, four, four, four, four, four, three, three, three, four),
        out_specs=(four, four, four, P()),
        check_vma=False,
    )
```
